32 devices in a mesh: beam: 2 (over y), tm: 4 (over z), sect: 2 (over x), pol: 2 (over core).
Axes of the slice: x: 2, y: 2, z: 4, core: 2. Of those that a mesh axis runs over, the one named last changes fastest.
Arguments:
- signal: float32 [2, 2, 512, 4096], P(None, 'pol', ('beam', 'tm', 'sect')), parts along dimension 2, may hold values from -6 to 6
- coarse_taps: float32 [16, 4096], replicated, may hold values from -1.5 to 1.5
- fine_taps: float32 [16, 1024], replicated, may hold values from -1.5 to 1.5
- channel_order: int32 [4096], replicated, may hold values from 0 to 4095, each once
Outputs:
- fine_spectra: float32 [2, 2, 8192, 1, 1024], P(None, 'pol', ('beam', 'tm', 'sect')), parts along dimension 2
The draws below stay inside these ranges and needn't reach their ends.
There are 2 independent parts, one for each index of `beam`. The reference program is written for one: setup_inputs(seed, part) draws one part's arguments, and reference() takes and returns one part's arrays. A program takes and returns all parts, laid end to end along the dimension named above; an argument that names none is the same for every part. Nothing has to cross between parts.
Inputs may be any that keep to these rules, and one draw needn't show every extreme that they name: `channel_order`: each of the 4096 coarse channels appears exactly once.
All inputs are finite; a program needn't handle non-finite values.
Results may differ from the reference program's by a relative error of at most 0.0001.
Values sent between devices are 32-bit elements; how exact they have to be, the bound alone decides.
A program may use at most 128 MiB of HBM per device.

```python
import jax
import jax.numpy as jnp
from jax import lax

COARSE = 4096
FINE = 1024
TAPS = 16
POL = 2
TSPEC = 256
FSPEC = 1


def block_scale(stream_key, shape, split, least, high):
    factor_of, own = 1.0, jax.random.fold_in(stream_key, 6)
    for position, parts in split:
        steps = jnp.exp(jax.random.uniform(jax.random.fold_in(own, position), (parts,), jnp.float32, least / len(split), high / len(split)))
        factor_of = factor_of * jnp.repeat(steps, shape[position] // parts).reshape([-1 if axis == position else 1 for axis in range(len(shape))])
    return factor_of


def gaussian(own_key, extent, width, reach, split=(), kind=jnp.bfloat16):
    gain = block_scale(own_key, extent, split, -0.22, 0.18) if split else 1.0
    result = jax.random.normal(own_key, extent, jnp.float32) * width * gain
    return jnp.minimum(jnp.maximum(result, -reach), reach).astype(kind)


def setup_inputs(seed: int = 0, part: int = 0) -> dict:
    key_of = jax.random.split(jax.random.key(seed), 5)
    part_keys = jax.random.split(jax.random.fold_in(key_of[4], part), 5)
    signal = gaussian(part_keys[0], (2, POL, TSPEC, COARSE), 1.0, 6.0, ((1, 2), (2, 8)), jnp.float32)
    coarse_taps = gaussian(key_of[1], (TAPS, COARSE), TAPS ** -0.5, 1.5, (), jnp.float32)
    fine_taps = gaussian(key_of[2], (TAPS, FINE), TAPS ** -0.5, 1.5, (), jnp.float32)
    channel_order = jax.random.permutation(key_of[3], COARSE).astype(jnp.int32)
    return dict(signal=signal, coarse_taps=coarse_taps, fine_taps=fine_taps, channel_order=channel_order)


def reference(signal, coarse_taps, fine_taps, channel_order):
    frame_count = TSPEC
    results = []
    for polar_index in range(signal.shape[1]):
        complex_slab = lax.complex(signal[0, polar_index], signal[1, polar_index])
        padded = jnp.concatenate([complex_slab, jnp.zeros((TAPS - 1, COARSE), complex_slab.dtype)], axis=0)
        filtered = coarse_taps[0] * padded[0:frame_count]
        for tap_index in range(1, TAPS):
            filtered = filtered + coarse_taps[tap_index] * padded[tap_index:tap_index + frame_count]
        coarse = jnp.fft.fft(filtered, axis=1, norm="ortho")
        series = jnp.take(coarse, channel_order, axis=1).T
        total_len = (FSPEC + TAPS - 1) * FINE
        series = jnp.pad(series, ((0, 0), (0, total_len - frame_count)))
        frames = series.reshape(COARSE, FSPEC + TAPS - 1, FINE)
        fine_filtered = fine_taps[0] * frames[:, 0:FSPEC]
        for tap_index in range(1, TAPS):
            fine_filtered = fine_filtered + fine_taps[tap_index] * frames[:, tap_index:tap_index + FSPEC]
        fine = jnp.fft.fft(fine_filtered, axis=2, norm="ortho")
        results.append(jnp.stack([jnp.real(fine), jnp.imag(fine)]))
    return jnp.stack(results, axis=1).astype(jnp.float32)
```

```python
from functools import partial
import math

import jax
import jax.numpy as jnp
import numpy as np
from jax import lax
from jax.experimental import pallas as pl
from jax.experimental.pallas import tpu as pltpu
from jax.sharding import PartitionSpec as P

LANES = 128
ROWS = 8
GROUP = ("tm", "sect")


def shifted(value, axis, steps):
    count = lax.axis_size(axis)
    initial, last = (max(0, -steps), min(count, count - steps))
    return lax.ppermute(value, axis, [(source, source + steps) for source in range(initial, last)])


def split_const(table):
    high = np.asarray(table, np.float32).astype(jnp.bfloat16)
    low = (np.asarray(table, np.float64) - high.astype(np.float64)).astype(jnp.bfloat16)
    return high, low


def split(value):
    high = value.astype(jnp.bfloat16)
    low = (value - high.astype(jnp.float32)).astype(jnp.bfloat16)
    return high, low


def dot3(high, low, table_high, table_low):
    product = partial(jnp.dot, preferred_element_type=jnp.float32)
    return product(high, table_high) + (product(low, table_high) + product(high, table_low))


def butterflies(points):
    count = len(points)
    if count == 1:
        return points
    even, odd = butterflies(points[0::2]), butterflies(points[1::2])
    first, second = [], []
    for k in range(count // 2):
        angle = -2.0 * math.pi * k / count
        cos, sin = math.cos(angle), math.sin(angle)
        (er, ei), (xr, xi) = even[k], odd[k]
        if k == 0:
            tr, ti = xr, xi
        elif 4 * k == count:
            tr, ti = xi, -xr
        else:
            tr, ti = xr * cos - xi * sin, xr * sin + xi * cos
        first.append((er + tr, ei + ti))
        second.append((er - tr, ei - ti))
    return first + second


def coarse_tables(width):
    chunks = width // LANES
    k, b = np.arange(chunks)[:, None], np.arange(LANES)[None, :]
    angle = 2.0 * np.pi * (k * b % width) / width
    twist = np.stack([np.cos(angle), -np.sin(angle)]).astype(np.float32)
    b, m = np.arange(LANES)[:, None], np.arange(LANES)[None, :]
    angle = 2.0 * np.pi * (b * m % LANES) / LANES
    cos, sin = np.cos(angle), np.sin(angle)
    matrix = np.block([[cos, -sin], [sin, cos]]) / math.sqrt(width)
    high, low = split_const(matrix)
    return twist, high, low


def fill(ext, source, first_row):
    chunks = ext.shape[1]
    rows = source.shape[1]
    for q in range(chunks):
        for c in range(2):
            ext[c, q, first_row : first_row + rows, :] = source[c, :, q * LANES : (q + 1) * LANES]


def spectra_rows(ext, taps_ref, twist_ref, high_ref, low_ref, filt, lhs, spec, start, rows):
    chunks = ext.shape[1]
    tap_count = taps_ref.shape[0]
    groups = rows // ROWS

    @pl.loop(0, chunks)
    def _(q):
        lanes = pl.ds(pl.multiple_of(q * LANES, LANES), LANES)
        sums = [[None] * groups for _ in range(2)]
        for k in range(tap_count):
            tap = jnp.broadcast_to(taps_ref[k : k + 1, lanes], (ROWS, LANES))
            for c in range(2):
                for g in range(groups):
                    term = tap * ext[c, q, start + g * ROWS + k : start + (g + 1) * ROWS + k, :]
                    sums[c][g] = term if k == 0 else sums[c][g] + term
        for c in range(2):
            for g in range(groups):
                filt[c, q, start + g * ROWS : start + (g + 1) * ROWS, :] = sums[c][g]

    @pl.loop(0, groups)
    def _(g):
        at = pl.ds(pl.multiple_of(start + g * ROWS, ROWS), ROWS)
        points = [(filt[0, q, at, :], filt[1, q, at, :]) for q in range(chunks)]
        for k, (re, im) in enumerate(butterflies(points)):
            wr, wi = twist_ref[0, k : k + 1, :], twist_ref[1, k : k + 1, :]
            lhs[k, at, 0:LANES] = re * wr - im * wi
            lhs[k, at, LANES : 2 * LANES] = re * wi + im * wr

    @pl.loop(0, chunks // 8)
    def _(j):
        part = pl.ds(j * 8, 8)
        value = lhs[part, start : start + rows, :].reshape(8 * rows, 2 * LANES)
        high, low = split(value)
        result = dot3(high, low, high_ref[...], low_ref[...])
        spec[part, start : start + rows, :] = result.reshape(8, rows, 2 * LANES)


def gathered(spec, place_ref, p, start, rows):
    chunks = spec.shape[0]
    place = jnp.broadcast_to(place_ref[pl.ds(p, 1), :], (ROWS, LANES))
    lane = place % LANES
    chunk = place // LANES
    keys = [(c, g) for c in range(2) for g in range(rows // ROWS)]
    sums = {}
    for q in range(chunks):
        mask = chunk == q
        for c, g in keys:
            source = spec[q, start + g * ROWS : start + (g + 1) * ROWS, c * LANES : (c + 1) * LANES]
            moved = jnp.take_along_axis(source, lane, axis=1, mode="promise_in_bounds")
            sums[c, g] = moved if q == 0 else jnp.where(mask, moved, sums[c, g])
    return sums


def coarse_kernel(signal_ref, next_ref, taps_ref, place_ref, twist_ref, high_ref, low_ref, out_ref, ext, filt, lhs, spec):
    rows = signal_ref.shape[1]
    fill(ext, signal_ref, 0)
    fill(ext, next_ref, rows)
    spectra_rows(ext, taps_ref, twist_ref, high_ref, low_ref, filt, lhs, spec, 0, rows)
    chunks = spec.shape[0]

    @pl.loop(0, chunks)
    def _(p):
        sums = gathered(spec, place_ref, p, 0, rows)
        for (c, g), value in sums.items():
            out_ref[p, c, g * ROWS : (g + 1) * ROWS, :] = value


def coarse_local(signal, next_rows, taps, place):
    _, rows, width = signal.shape
    chunks = width // LANES
    twist, high, low = coarse_tables(width)
    lead = next_rows.shape[1]
    return pl.pallas_call(
        coarse_kernel,
        out_shape=jax.ShapeDtypeStruct((chunks, 2, rows, LANES), jnp.float32),
        in_specs=[pl.BlockSpec(memory_space=pltpu.VMEM)] * 7,
        out_specs=pl.BlockSpec(memory_space=pltpu.VMEM),
        scratch_shapes=[
            pltpu.VMEM((2, chunks, rows + lead, LANES), jnp.float32),
            pltpu.VMEM((2, chunks, rows, LANES), jnp.float32),
            pltpu.VMEM((chunks, rows, 2 * LANES), jnp.float32),
            pltpu.VMEM((chunks, rows, 2 * LANES), jnp.float32),
        ],
        name="coarse",
    )(signal, next_rows, taps, place, twist, high, low)


def fine_kernel(arrived_ref, taps_ref, cos_high, cos_low, sin_high, sin_low, out_ref):
    sources, slot_chunks, _, rows, slots = arrived_ref.shape
    length = sources * rows
    width = cos_high.shape[1]
    high, low = [], []
    for c in range(2):
        series = arrived_ref[:, 0, c].reshape(length, slots)
        filtered = series.T * taps_ref[...]
        parts = split(filtered)
        high.append(parts[0])
        low.append(parts[1])
    high = jnp.concatenate(high, axis=0)
    low = jnp.concatenate(low, axis=0)
    per_slot = width // LANES
    step = 2 * LANES
    for m in range(width // step):
        lanes = slice(m * step, (m + 1) * step)
        with_cos = dot3(high, low, cos_high[:, lanes], cos_low[:, lanes])
        with_sin = dot3(high, low, sin_high[:, lanes], sin_low[:, lanes])
        re = with_cos[:slots] + with_sin[slots:]
        im = with_cos[slots:] - with_sin[:slots]
        for h in range(2):
            at = pl.ds(m * 2 + h, slots, stride=per_slot)
            out_ref[0, at, :] = re[:, h * LANES : (h + 1) * LANES]
            out_ref[1, at, :] = im[:, h * LANES : (h + 1) * LANES]


def fine_local(arrived, fine_taps):
    sources, slot_chunks, _, rows, slots = arrived.shape
    length = sources * rows
    width = fine_taps.shape[1]
    j, m = np.arange(length)[:, None], np.arange(width)[None, :]
    angle = 2.0 * np.pi * (j * m % width) / width
    scale = 1.0 / math.sqrt(width)
    tables = split_const(np.cos(angle) * scale) + split_const(np.sin(angle) * scale)
    per_slot = width // LANES
    whole = lambda shape: pl.BlockSpec(shape, lambda i: (0, 0))
    out = pl.pallas_call(
        fine_kernel,
        grid=(slot_chunks,),
        out_shape=jax.ShapeDtypeStruct((2, slot_chunks * slots * per_slot, LANES), jnp.float32),
        in_specs=[
            pl.BlockSpec((sources, 1, 2, rows, slots), lambda i: (0, i, 0, 0, 0)),
            whole((1, length)),
        ]
        + [whole((length, width))] * 4,
        out_specs=pl.BlockSpec((2, slots * per_slot, LANES), lambda i: (0, i, 0)),
        name="fine",
    )(arrived, fine_taps[0:1, :length], *tables)
    return out.reshape(2, 1, slot_chunks * slots, 1, width)


def fine_general(series, fine_taps):
    slots, total_len = series.shape[1:]
    tap_count, width = fine_taps.shape
    frames = -(-total_len // width)
    blocks = jnp.pad(series, ((0, 0), (0, 0), (0, frames * width - total_len)))
    blocks = blocks.reshape(2, slots, frames, width)
    filtered = fine_taps[0] * blocks
    for k in range(1, min(tap_count, frames)):
        term = fine_taps[k] * blocks[:, :, k:]
        filtered = filtered + jnp.pad(term, ((0, 0), (0, 0), (0, k), (0, 0)))
    j, m = np.arange(width)[:, None], np.arange(width)[None, :]
    angle = 2.0 * np.pi * (j * m % width) / width
    scale = 1.0 / math.sqrt(width)
    cos = jnp.asarray((np.cos(angle) * scale).astype(np.float32))
    sin = jnp.asarray((np.sin(angle) * scale).astype(np.float32))
    product = partial(jnp.einsum, "snfj,jm->snfm", precision=lax.Precision.HIGHEST)
    with_cos, with_sin = product(filtered, cos), product(filtered, sin)
    return jnp.stack([with_cos[0] + with_sin[1], with_cos[1] - with_sin[0]])[:, None]


def body(signal, coarse_taps, fine_taps, channel_order):
    signal = signal[:, 0]
    slab_len, width = signal.shape[1:]
    tap_count = coarse_taps.shape[0]
    chunks = width // LANES
    owners = lax.axis_size(GROUP)
    own_count = width // owners
    place = (channel_order % chunks * LANES + channel_order // chunks).reshape(chunks, LANES)
    lead = -(-(tap_count - 1) // ROWS) * ROWS
    next_rows = shifted(signal[:, :lead], GROUP, -1)
    ordered = coarse_local(signal, next_rows, coarse_taps, place)
    total_len = owners * slab_len
    if own_count % LANES == 0 and total_len <= fine_taps.shape[1]:
        blocks = ordered.reshape(owners, own_count // LANES, 2, slab_len, LANES)
        arrived = lax.all_to_all(blocks, GROUP, split_axis=0, concat_axis=0, tiled=True)
        return fine_local(arrived, fine_taps)
    blocks = ordered.transpose(0, 3, 1, 2).reshape(owners, own_count, 2, slab_len)
    arrived = lax.all_to_all(blocks, GROUP, split_axis=0, concat_axis=0, tiled=True)
    series = arrived.transpose(2, 1, 0, 3).reshape(2, own_count, total_len)
    return fine_general(series, fine_taps)


def solution(mesh):
    in_specs = (P(None, "pol", ("beam", "tm", "sect"), None), P(), P(), P())
    out_specs = P(None, "pol", ("beam", "tm", "sect"), None, None)
    return jax.shard_map(body, mesh=mesh, in_specs=in_specs, out_specs=out_specs, check_vma=False)
```

```python
from functools import partial
import math

import jax
import jax.numpy as jnp
import numpy as np
from jax import lax
from jax.experimental import pallas as pl
from jax.experimental.pallas import tpu as pltpu
from jax.sharding import PartitionSpec as P

LANES = 128
ROWS = 8
GROUP = ("tm", "sect")
PHASES = 2


def shifted(value, axis, steps):
    count = lax.axis_size(axis)
    initial, last = (max(0, -steps), min(count, count - steps))
    return lax.ppermute(value, axis, [(source, source + steps) for source in range(initial, last)])


def split_const(table):
    high = np.asarray(table, np.float32).astype(jnp.bfloat16)
    low = (np.asarray(table, np.float64) - high.astype(np.float64)).astype(jnp.bfloat16)
    return high, low


def split(value):
    high = value.astype(jnp.bfloat16)
    low = (value - high.astype(jnp.float32)).astype(jnp.bfloat16)
    return high, low


def dot3(high, low, table_high, table_low):
    product = partial(jnp.dot, preferred_element_type=jnp.float32)
    return product(high, table_high) + (product(low, table_high) + product(high, table_low))


def butterflies(points):
    count = len(points)
    if count == 1:
        return points
    even, odd = butterflies(points[0::2]), butterflies(points[1::2])
    first, second = [], []
    for k in range(count // 2):
        angle = -2.0 * math.pi * k / count
        cos, sin = math.cos(angle), math.sin(angle)
        (er, ei), (xr, xi) = even[k], odd[k]
        if k == 0:
            tr, ti = xr, xi
        elif 4 * k == count:
            tr, ti = xi, -xr
        else:
            tr, ti = xr * cos - xi * sin, xr * sin + xi * cos
        first.append((er + tr, ei + ti))
        second.append((er - tr, ei - ti))
    return first + second


def coarse_tables(width):
    chunks = width // LANES
    k, b = np.arange(chunks)[:, None], np.arange(LANES)[None, :]
    angle = 2.0 * np.pi * (k * b % width) / width
    twist = np.stack([np.cos(angle), -np.sin(angle)]).astype(np.float32)
    b, m = np.arange(LANES)[:, None], np.arange(LANES)[None, :]
    angle = 2.0 * np.pi * (b * m % LANES) / LANES
    cos, sin = np.cos(angle), np.sin(angle)
    matrix = np.block([[cos, -sin], [sin, cos]]) / math.sqrt(width)
    high, low = split_const(matrix)
    return twist, high, low


def fill(ext, source, first_row):
    chunks = ext.shape[1]
    rows = source.shape[1]
    for q in range(chunks):
        for c in range(2):
            ext[c, q, first_row : first_row + rows, :] = source[c, :, q * LANES : (q + 1) * LANES]


def spectra_rows(ext, taps_ref, twist_ref, high_ref, low_ref, filt, lhs, spec, start, rows):
    chunks = ext.shape[1]
    tap_count = taps_ref.shape[0]
    groups = rows // ROWS

    @pl.loop(0, chunks)
    def _(q):
        lanes = pl.ds(pl.multiple_of(q * LANES, LANES), LANES)
        sums = [[None] * groups for _ in range(2)]
        for k in range(tap_count):
            tap = jnp.broadcast_to(taps_ref[k : k + 1, lanes], (ROWS, LANES))
            for c in range(2):
                for g in range(groups):
                    term = tap * ext[c, q, start + g * ROWS + k : start + (g + 1) * ROWS + k, :]
                    sums[c][g] = term if k == 0 else sums[c][g] + term
        for c in range(2):
            for g in range(groups):
                filt[c, q, start + g * ROWS : start + (g + 1) * ROWS, :] = sums[c][g]

    @pl.loop(0, groups)
    def _(g):
        at = pl.ds(pl.multiple_of(start + g * ROWS, ROWS), ROWS)
        points = [(filt[0, q, at, :], filt[1, q, at, :]) for q in range(chunks)]
        for k, (re, im) in enumerate(butterflies(points)):
            wr, wi = twist_ref[0, k : k + 1, :], twist_ref[1, k : k + 1, :]
            lhs[k, at, 0:LANES] = re * wr - im * wi
            lhs[k, at, LANES : 2 * LANES] = re * wi + im * wr

    @pl.loop(0, chunks // 8)
    def _(j):
        part = pl.ds(j * 8, 8)
        value = lhs[part, start : start + rows, :].reshape(8 * rows, 2 * LANES)
        high, low = split(value)
        result = dot3(high, low, high_ref[...], low_ref[...])
        spec[part, start : start + rows, :] = result.reshape(8, rows, 2 * LANES)


def gathered(spec, place_ref, p, start, rows):
    chunks = spec.shape[0]
    channel = jnp.broadcast_to(place_ref[pl.ds(p, 1), :], (ROWS, LANES))
    lane = lax.div(channel, chunks)
    chunk = channel - lane * chunks
    keys = [(c, g) for c in range(2) for g in range(rows // ROWS)]
    sums = {}
    for q in range(chunks):
        mask = chunk == q
        for c, g in keys:
            source = spec[q, start + g * ROWS : start + (g + 1) * ROWS, c * LANES : (c + 1) * LANES]
            moved = jnp.take_along_axis(source, lane, axis=1, mode="promise_in_bounds")
            sums[c, g] = moved if q == 0 else jnp.where(mask, moved, sums[c, g])
    return sums


def coarse_kernel(signal_ref, next_ref, taps_ref, place_ref, twist_ref, high_ref, low_ref, out_ref, ext, filt, lhs, spec):
    rows = signal_ref.shape[1]
    fill(ext, signal_ref, 0)
    fill(ext, next_ref, rows)
    spectra_rows(ext, taps_ref, twist_ref, high_ref, low_ref, filt, lhs, spec, 0, rows)
    chunks = spec.shape[0]

    @pl.loop(0, chunks)
    def _(p):
        sums = gathered(spec, place_ref, p, 0, rows)
        for (c, g), value in sums.items():
            out_ref[p, c, g * ROWS : (g + 1) * ROWS, :] = value


def coarse_local(signal, next_rows, taps, place):
    _, rows, width = signal.shape
    chunks = width // LANES
    twist, high, low = coarse_tables(width)
    lead = next_rows.shape[1]
    return pl.pallas_call(
        coarse_kernel,
        out_shape=jax.ShapeDtypeStruct((chunks, 2, rows, LANES), jnp.float32),
        in_specs=[pl.BlockSpec(memory_space=pltpu.VMEM)] * 7,
        out_specs=pl.BlockSpec(memory_space=pltpu.VMEM),
        scratch_shapes=[
            pltpu.VMEM((2, chunks, rows + lead, LANES), jnp.float32),
            pltpu.VMEM((2, chunks, rows, LANES), jnp.float32),
            pltpu.VMEM((chunks, rows, 2 * LANES), jnp.float32),
            pltpu.VMEM((chunks, rows, 2 * LANES), jnp.float32),
        ],
        name="coarse",
    )(signal, next_rows, taps, place, twist, high, low)


def exchange_kernel(
    signal_ref, taps_ref, place_ref, twist_ref, high_ref, low_ref, out_ref,
    halo, ext, filt, lhs, spec, stage, halo_send, halo_recv, send_sem, recv_sem, own_sem,
):
    tms, sects = lax.axis_size("tm"), lax.axis_size("sect")
    owners = tms * sects
    tm, sect = lax.axis_index("tm"), lax.axis_index("sect")
    me = tm * sects + sect
    chunks = spec.shape[0]
    slot_chunks = chunks // owners
    slab_len = signal_ref.shape[1]
    rows = slab_len // PHASES
    lead = halo.shape[1]

    def device(index):
        return {"tm": lax.div(index, sects), "sect": lax.rem(index, sects)}

    barrier = pltpu.get_barrier_semaphore()
    for offset in range(1, owners):
        peer = lax.rem(me + offset, owners)
        pl.semaphore_signal(barrier, inc=1, device_id=device(peer), device_id_type=pl.DeviceIdType.MESH)
    pl.semaphore_wait(barrier, owners - 1)

    halo_copy = pltpu.make_async_remote_copy(
        src_ref=signal_ref.at[:, 0:lead, :],
        dst_ref=halo,
        send_sem=halo_send,
        recv_sem=halo_recv,
        device_id=device(lax.rem(me + owners - 1, owners)),
        device_id_type=pl.DeviceIdType.MESH,
    )

    @pl.when(me > 0)
    def _():
        halo_copy.start()

    def block_copy(phase, owner, source):
        return pltpu.make_async_remote_copy(
            src_ref=stage.at[owner, phase],
            dst_ref=out_ref.at[source, phase],
            send_sem=send_sem.at[phase, owner],
            recv_sem=recv_sem.at[phase, source],
            device_id=device(owner),
            device_id_type=pl.DeviceIdType.MESH,
        )

    fill(ext, signal_ref, 0)
    for phase in range(PHASES):
        start = phase * rows
        if phase == PHASES - 1:

            @pl.when(me < owners - 1)
            def _():
                halo_copy.wait_recv()
                fill(ext, halo, slab_len)

            @pl.when(me == owners - 1)
            def _():
                ext[:, :, slab_len:, :] = jnp.zeros((2, chunks, lead, LANES), jnp.float32)

        spectra_rows(ext, taps_ref, twist_ref, high_ref, low_ref, filt, lhs, spec, start, rows)

        @pl.loop(0, owners)
        def _(step):
            turn = lax.div(step, sects)
            half = tms // 2
            turn = jnp.where(turn < tms - half, half + turn, tms - 1 - turn)
            owner = lax.rem(tm + turn, tms) * sects + lax.rem(sect + 1 + step, sects)

            @pl.loop(0, slot_chunks)
            def _(i):
                sums = gathered(spec, place_ref, owner * slot_chunks + i, start, rows)
                for (c, g), value in sums.items():
                    stage[owner, phase, i, c, g * ROWS : (g + 1) * ROWS, :] = value

            @pl.when(owner != me)
            def _():
                block_copy(phase, owner, me).start()

    own_copy = pltpu.make_async_copy(stage.at[me], out_ref.at[me], own_sem)
    own_copy.start()
    own_copy.wait()

    @pl.when(me > 0)
    def _():
        halo_copy.wait_send()

    for phase in range(PHASES):

        @pl.loop(1, owners)
        def _(offset):
            peer = lax.rem(me + offset, owners)
            copy = block_copy(phase, peer, peer)
            copy.wait_send()
            copy.wait_recv()


def coarse_exchange(signal, taps, place):
    _, rows, width = signal.shape
    chunks = width // LANES
    owners = lax.axis_size(GROUP)
    twist, high, low = coarse_tables(width)
    lead = rows // PHASES
    blocks = (owners, PHASES, chunks // owners, 2, lead, LANES)
    return pl.pallas_call(
        exchange_kernel,
        out_shape=jax.ShapeDtypeStruct(blocks, jnp.float32),
        in_specs=[pl.BlockSpec(memory_space=pltpu.VMEM)] * 6,
        out_specs=pl.BlockSpec(memory_space=pl.ANY),
        scratch_shapes=[
            pltpu.VMEM((2, lead, width), jnp.float32),
            pltpu.VMEM((2, chunks, rows + lead, LANES), jnp.float32),
            pltpu.VMEM((2, chunks, rows, LANES), jnp.float32),
            pltpu.VMEM((chunks, rows, 2 * LANES), jnp.float32),
            pltpu.VMEM((chunks, rows, 2 * LANES), jnp.float32),
            pltpu.VMEM(blocks, jnp.float32),
            pltpu.SemaphoreType.DMA,
            pltpu.SemaphoreType.DMA,
            pltpu.SemaphoreType.DMA((PHASES, owners)),
            pltpu.SemaphoreType.DMA((PHASES, owners)),
            pltpu.SemaphoreType.DMA,
        ],
        compiler_params=pltpu.CompilerParams(collective_id=0, has_side_effects=True),
        name="exchange",
    )(signal, taps, place, twist, high, low)


def fine_kernel(arrived_ref, taps_ref, cos_high, cos_low, sin_high, sin_low, out_ref):
    sources, slot_chunks, _, rows, slots = arrived_ref.shape
    length = sources * rows
    width = cos_high.shape[1]
    high, low = [], []
    for c in range(2):
        series = arrived_ref[:, 0, c].reshape(length, slots)
        filtered = series.T * taps_ref[0:1, :length]
        parts = split(filtered)
        high.append(parts[0])
        low.append(parts[1])
    high = jnp.concatenate(high, axis=0)
    low = jnp.concatenate(low, axis=0)
    per_slot = width // LANES
    step = 2 * LANES
    for m in range(width // step):
        lanes = slice(m * step, (m + 1) * step)
        with_cos = dot3(high, low, cos_high[:, lanes], cos_low[:, lanes])
        with_sin = dot3(high, low, sin_high[:, lanes], sin_low[:, lanes])
        re = with_cos[:slots] + with_sin[slots:]
        im = with_cos[slots:] - with_sin[:slots]
        for h in range(2):
            at = pl.ds(m * 2 + h, slots, stride=per_slot)
            out_ref[0, at, :] = re[:, h * LANES : (h + 1) * LANES]
            out_ref[1, at, :] = im[:, h * LANES : (h + 1) * LANES]


def fine_local(arrived, fine_taps):
    sources, slot_chunks, _, rows, slots = arrived.shape
    length = sources * rows
    width = fine_taps.shape[1]
    j, m = np.arange(length)[:, None], np.arange(width)[None, :]
    angle = 2.0 * np.pi * (j * m % width) / width
    scale = 1.0 / math.sqrt(width)
    tables = split_const(np.cos(angle) * scale) + split_const(np.sin(angle) * scale)
    per_slot = width // LANES
    whole = lambda shape: pl.BlockSpec(shape, lambda i: (0, 0))
    out = pl.pallas_call(
        fine_kernel,
        grid=(slot_chunks,),
        out_shape=jax.ShapeDtypeStruct((2, slot_chunks * slots * per_slot, LANES), jnp.float32),
        in_specs=[
            pl.BlockSpec((sources, 1, 2, rows, slots), lambda i: (0, i, 0, 0, 0)),
            whole(fine_taps.shape),
        ]
        + [whole((length, width))] * 4,
        out_specs=pl.BlockSpec((2, slots * per_slot, LANES), lambda i: (0, i, 0)),
        name="fine",
    )(arrived, fine_taps, *tables)
    return out.reshape(2, 1, slot_chunks * slots, 1, width)


def fine_general(series, fine_taps):
    slots, total_len = series.shape[1:]
    tap_count, width = fine_taps.shape
    frames = -(-total_len // width)
    blocks = jnp.pad(series, ((0, 0), (0, 0), (0, frames * width - total_len)))
    blocks = blocks.reshape(2, slots, frames, width)
    filtered = fine_taps[0] * blocks
    for k in range(1, min(tap_count, frames)):
        term = fine_taps[k] * blocks[:, :, k:]
        filtered = filtered + jnp.pad(term, ((0, 0), (0, 0), (0, k), (0, 0)))
    j, m = np.arange(width)[:, None], np.arange(width)[None, :]
    angle = 2.0 * np.pi * (j * m % width) / width
    scale = 1.0 / math.sqrt(width)
    cos = jnp.asarray((np.cos(angle) * scale).astype(np.float32))
    sin = jnp.asarray((np.sin(angle) * scale).astype(np.float32))
    product = partial(jnp.einsum, "snfj,jm->snfm", precision=lax.Precision.HIGHEST)
    with_cos, with_sin = product(filtered, cos), product(filtered, sin)
    return jnp.stack([with_cos[0] + with_sin[1], with_cos[1] - with_sin[0]])[:, None]


def body(signal, coarse_taps, fine_taps, channel_order):
    signal = signal[:, 0]
    slab_len, width = signal.shape[1:]
    tap_count = coarse_taps.shape[0]
    chunks = width // LANES
    owners = lax.axis_size(GROUP)
    own_count = width // owners
    place = channel_order.reshape(chunks, LANES)
    lead = -(-(tap_count - 1) // ROWS) * ROWS
    total_len = owners * slab_len
    if own_count % LANES == 0 and total_len <= fine_taps.shape[1] and slab_len == PHASES * lead:
        arrived = coarse_exchange(signal, coarse_taps, place)
        return fine_local(arrived.reshape(-1, *arrived.shape[2:]), fine_taps)
    next_rows = shifted(signal[:, :lead], GROUP, -1)
    ordered = coarse_local(signal, next_rows, coarse_taps, place)
    blocks = ordered.transpose(0, 3, 1, 2).reshape(owners, own_count, 2, slab_len)
    arrived = lax.all_to_all(blocks, GROUP, split_axis=0, concat_axis=0, tiled=True)
    series = arrived.transpose(2, 1, 0, 3).reshape(2, own_count, total_len)
    return fine_general(series, fine_taps)


def solution(mesh):
    in_specs = (P(None, "pol", ("beam", "tm", "sect"), None), P(), P(), P())
    out_specs = P(None, "pol", ("beam", "tm", "sect"), None, None)
    return jax.shard_map(body, mesh=mesh, in_specs=in_specs, out_specs=out_specs, check_vma=False)
```

```python
from functools import partial
import math

import jax
import jax.numpy as jnp
import numpy as np
from jax import lax
from jax.experimental import pallas as pl
from jax.experimental.pallas import tpu as pltpu
from jax.sharding import PartitionSpec as P

LANES = 128
ROWS = 8
GROUP = ("tm", "sect")


def shifted(value, axis, steps):
    count = lax.axis_size(axis)
    initial, last = (max(0, -steps), min(count, count - steps))
    return lax.ppermute(value, axis, [(source, source + steps) for source in range(initial, last)])


def split_const(table):
    high = np.asarray(table, np.float32).astype(jnp.bfloat16)
    low = (np.asarray(table, np.float64) - high.astype(np.float64)).astype(jnp.bfloat16)
    return high, low


def split(value):
    high = value.astype(jnp.bfloat16)
    low = (value - high.astype(jnp.float32)).astype(jnp.bfloat16)
    return high, low


def dot3(high, low, table_high, table_low):
    product = partial(jnp.dot, preferred_element_type=jnp.float32)
    return product(high, table_high) + (product(low, table_high) + product(high, table_low))


def butterflies(points):
    count = len(points)
    if count == 1:
        return points
    even, odd = butterflies(points[0::2]), butterflies(points[1::2])
    first, second = [], []
    for k in range(count // 2):
        angle = -2.0 * math.pi * k / count
        cos, sin = math.cos(angle), math.sin(angle)
        (er, ei), (xr, xi) = even[k], odd[k]
        if k == 0:
            tr, ti = xr, xi
        elif 4 * k == count:
            tr, ti = xi, -xr
        else:
            tr, ti = xr * cos - xi * sin, xr * sin + xi * cos
        first.append((er + tr, ei + ti))
        second.append((er - tr, ei - ti))
    return first + second


def coarse_tables(width):
    chunks = width // LANES
    k, b = np.arange(chunks)[:, None], np.arange(LANES)[None, :]
    angle = 2.0 * np.pi * (k * b % width) / width
    twist = np.stack([np.cos(angle), -np.sin(angle)]).astype(np.float32)
    b, m = np.arange(LANES)[:, None], np.arange(LANES)[None, :]
    angle = 2.0 * np.pi * (b * m % LANES) / LANES
    cos, sin = np.cos(angle), np.sin(angle)
    matrix = np.block([[cos, -sin], [sin, cos]]) / math.sqrt(width)
    high, low = split_const(matrix)
    return twist, high, low


def fill(ext, source, first_row):
    chunks = ext.shape[1]
    rows = source.shape[1]
    for q in range(chunks):
        for c in range(2):
            ext[c, q, first_row : first_row + rows, :] = source[c, :, q * LANES : (q + 1) * LANES]


def spectra_rows(ext, taps_ref, twist_ref, high_ref, low_ref, filt, lhs, spec, start, rows):
    chunks = ext.shape[1]
    tap_count = taps_ref.shape[0]
    groups = rows // ROWS

    @pl.loop(0, chunks)
    def _(q):
        lanes = pl.ds(pl.multiple_of(q * LANES, LANES), LANES)
        sums = [[None] * groups for _ in range(2)]
        for k in range(tap_count):
            tap = jnp.broadcast_to(taps_ref[k : k + 1, lanes], (ROWS, LANES))
            for c in range(2):
                for g in range(groups):
                    term = tap * ext[c, q, start + g * ROWS + k : start + (g + 1) * ROWS + k, :]
                    sums[c][g] = term if k == 0 else sums[c][g] + term
        for c in range(2):
            for g in range(groups):
                filt[c, q, start + g * ROWS : start + (g + 1) * ROWS, :] = sums[c][g]

    @pl.loop(0, groups)
    def _(g):
        at = pl.ds(pl.multiple_of(start + g * ROWS, ROWS), ROWS)
        points = [(filt[0, q, at, :], filt[1, q, at, :]) for q in range(chunks)]
        for k, (re, im) in enumerate(butterflies(points)):
            wr, wi = twist_ref[0, k : k + 1, :], twist_ref[1, k : k + 1, :]
            lhs[k, at, 0:LANES] = re * wr - im * wi
            lhs[k, at, LANES : 2 * LANES] = re * wi + im * wr

    @pl.loop(0, chunks // 8)
    def _(j):
        part = pl.ds(j * 8, 8)
        value = lhs[part, start : start + rows, :].reshape(8 * rows, 2 * LANES)
        high, low = split(value)
        result = dot3(high, low, high_ref[...], low_ref[...])
        spec[part, start : start + rows, :] = result.reshape(8, rows, 2 * LANES)


def gathered(spec, place_ref, p, start, rows):
    chunks = spec.shape[0]
    channel = jnp.broadcast_to(place_ref[pl.ds(p, 1), :], (ROWS, LANES))
    lane = lax.div(channel, chunks)
    chunk = channel - lane * chunks
    keys = [(c, g) for c in range(2) for g in range(rows // ROWS)]
    sums = {}
    for q in range(chunks):
        mask = chunk == q
        for c, g in keys:
            source = spec[q, start + g * ROWS : start + (g + 1) * ROWS, c * LANES : (c + 1) * LANES]
            moved = jnp.take_along_axis(source, lane, axis=1, mode="promise_in_bounds")
            sums[c, g] = moved if q == 0 else jnp.where(mask, moved, sums[c, g])
    return sums


def coarse_kernel(signal_ref, next_ref, taps_ref, place_ref, twist_ref, high_ref, low_ref, out_ref, ext, filt, lhs, spec):
    rows = signal_ref.shape[1]
    fill(ext, signal_ref, 0)
    fill(ext, next_ref, rows)
    spectra_rows(ext, taps_ref, twist_ref, high_ref, low_ref, filt, lhs, spec, 0, rows)
    chunks = spec.shape[0]

    @pl.loop(0, chunks)
    def _(p):
        sums = gathered(spec, place_ref, p, 0, rows)
        for (c, g), value in sums.items():
            out_ref[p, c, g * ROWS : (g + 1) * ROWS, :] = value


def coarse_local(signal, next_rows, taps, place):
    _, rows, width = signal.shape
    chunks = width // LANES
    twist, high, low = coarse_tables(width)
    lead = next_rows.shape[1]
    return pl.pallas_call(
        coarse_kernel,
        out_shape=jax.ShapeDtypeStruct((chunks, 2, rows, LANES), jnp.float32),
        in_specs=[pl.BlockSpec(memory_space=pltpu.VMEM)] * 7,
        out_specs=pl.BlockSpec(memory_space=pltpu.VMEM),
        scratch_shapes=[
            pltpu.VMEM((2, chunks, rows + lead, LANES), jnp.float32),
            pltpu.VMEM((2, chunks, rows, LANES), jnp.float32),
            pltpu.VMEM((chunks, rows, 2 * LANES), jnp.float32),
            pltpu.VMEM((chunks, rows, 2 * LANES), jnp.float32),
        ],
        name="coarse",
    )(signal, next_rows, taps, place, twist, high, low)


def exchange_kernel(
    signal_ref, taps_ref, place_ref, twist_ref, high_ref, low_ref, out_ref,
    halo, ext, filt, lhs, spec, stage, halo_send, halo_recv, send_sem, recv_sem, own_sem,
):
    tms, sects = lax.axis_size("tm"), lax.axis_size("sect")
    owners = tms * sects
    tm, sect = lax.axis_index("tm"), lax.axis_index("sect")
    me = tm * sects + sect
    chunks = spec.shape[0]
    slot_chunks = chunks // owners
    slab_len = signal_ref.shape[1]
    rows = ROWS
    phases = slab_len // rows
    reach = taps_ref.shape[0] - 1
    parts = halo.shape[0]

    def device(index):
        return {"tm": lax.div(index, sects), "sect": lax.rem(index, sects)}

    barrier = pltpu.get_barrier_semaphore()
    for offset in range(1, owners):
        peer = lax.rem(me + offset, owners)
        pl.semaphore_signal(barrier, inc=1, device_id=device(peer), device_id_type=pl.DeviceIdType.MESH)
    pl.semaphore_wait(barrier, owners - 1)

    def halo_copy(part):
        return pltpu.make_async_remote_copy(
            src_ref=signal_ref.at[:, part * ROWS : (part + 1) * ROWS, :],
            dst_ref=halo.at[part],
            send_sem=halo_send.at[part],
            recv_sem=halo_recv.at[part],
            device_id=device(lax.rem(me + owners - 1, owners)),
            device_id_type=pl.DeviceIdType.MESH,
        )

    @pl.when(me > 0)
    def _():
        for part in range(parts):
            halo_copy(part).start()

    def block_copy(phase, owner, source):
        return pltpu.make_async_remote_copy(
            src_ref=stage.at[owner, phase],
            dst_ref=out_ref.at[source, phase],
            send_sem=send_sem.at[phase, owner],
            recv_sem=recv_sem.at[phase, source],
            device_id=device(owner),
            device_id_type=pl.DeviceIdType.MESH,
        )

    fill(ext, signal_ref, 0)
    taken = 0
    for phase in range(phases):
        start = phase * rows
        needed = -(-(start + rows + reach - slab_len) // ROWS)
        for part in range(taken, needed):
            at = slab_len + part * ROWS

            @pl.when(me < owners - 1)
            def _():
                halo_copy(part).wait_recv()
                fill(ext, halo.at[part], at)

            @pl.when(me == owners - 1)
            def _():
                ext[:, :, at : at + ROWS, :] = jnp.zeros((2, chunks, ROWS, LANES), jnp.float32)

        taken = max(taken, needed)
        spectra_rows(ext, taps_ref, twist_ref, high_ref, low_ref, filt, lhs, spec, start, rows)

        @pl.loop(0, owners)
        def _(step):
            half = tms // 2
            if phase < phases - parts:
                turn = lax.rem(step, tms)
                to_sect = lax.rem(sect + lax.div(step, tms), sects)
            else:
                turn = lax.div(step, sects)
                to_sect = lax.rem(sect + 1 + step, sects)
            turn = jnp.where(turn < tms - half, half + turn, tms - 1 - turn)
            owner = lax.rem(tm + turn, tms) * sects + to_sect

            @pl.loop(0, slot_chunks)
            def _(i):
                sums = gathered(spec, place_ref, owner * slot_chunks + i, start, rows)
                for (c, g), value in sums.items():
                    stage[owner, phase, i, c, g * ROWS : (g + 1) * ROWS, :] = value

            @pl.when(owner != me)
            def _():
                block_copy(phase, owner, me).start()

    own_copy = pltpu.make_async_copy(stage.at[me], out_ref.at[me], own_sem)
    own_copy.start()
    own_copy.wait()

    @pl.when(me > 0)
    def _():
        for part in range(parts):
            halo_copy(part).wait_send()

    for phase in range(phases):

        @pl.loop(1, owners)
        def _(offset):
            peer = lax.rem(me + offset, owners)
            copy = block_copy(phase, peer, peer)
            copy.wait_send()
            copy.wait_recv()


def coarse_exchange(signal, taps, place):
    _, rows, width = signal.shape
    chunks = width // LANES
    owners = lax.axis_size(GROUP)
    twist, high, low = coarse_tables(width)
    parts = -(-(taps.shape[0] - 1) // ROWS)
    phases = rows // ROWS
    blocks = (owners, phases, chunks // owners, 2, ROWS, LANES)
    return pl.pallas_call(
        exchange_kernel,
        out_shape=jax.ShapeDtypeStruct(blocks, jnp.float32),
        in_specs=[pl.BlockSpec(memory_space=pltpu.VMEM)] * 6,
        out_specs=pl.BlockSpec(memory_space=pl.ANY),
        scratch_shapes=[
            pltpu.VMEM((parts, 2, ROWS, width), jnp.float32),
            pltpu.VMEM((2, chunks, rows + parts * ROWS, LANES), jnp.float32),
            pltpu.VMEM((2, chunks, rows, LANES), jnp.float32),
            pltpu.VMEM((chunks, rows, 2 * LANES), jnp.float32),
            pltpu.VMEM((chunks, rows, 2 * LANES), jnp.float32),
            pltpu.VMEM(blocks, jnp.float32),
            pltpu.SemaphoreType.DMA((parts,)),
            pltpu.SemaphoreType.DMA((parts,)),
            pltpu.SemaphoreType.DMA((phases, owners)),
            pltpu.SemaphoreType.DMA((phases, owners)),
            pltpu.SemaphoreType.DMA,
        ],
        compiler_params=pltpu.CompilerParams(collective_id=0, has_side_effects=True),
        name="exchange",
    )(signal, taps, place, twist, high, low)


def fine_kernel(arrived_ref, taps_ref, cos_high, cos_low, sin_high, sin_low, out_ref):
    sources, slot_chunks, _, rows, slots = arrived_ref.shape
    length = sources * rows
    width = cos_high.shape[1]
    high, low = [], []
    for c in range(2):
        series = arrived_ref[:, 0, c].reshape(length, slots)
        filtered = series.T * taps_ref[0:1, :length]
        parts = split(filtered)
        high.append(parts[0])
        low.append(parts[1])
    high = jnp.concatenate(high, axis=0)
    low = jnp.concatenate(low, axis=0)
    per_slot = width // LANES
    step = 2 * LANES
    for m in range(width // step):
        lanes = slice(m * step, (m + 1) * step)
        with_cos = dot3(high, low, cos_high[:, lanes], cos_low[:, lanes])
        with_sin = dot3(high, low, sin_high[:, lanes], sin_low[:, lanes])
        re = with_cos[:slots] + with_sin[slots:]
        im = with_cos[slots:] - with_sin[:slots]
        for h in range(2):
            at = pl.ds(m * 2 + h, slots, stride=per_slot)
            out_ref[0, at, :] = re[:, h * LANES : (h + 1) * LANES]
            out_ref[1, at, :] = im[:, h * LANES : (h + 1) * LANES]


def fine_local(arrived, fine_taps):
    sources, slot_chunks, _, rows, slots = arrived.shape
    length = sources * rows
    width = fine_taps.shape[1]
    j, m = np.arange(length)[:, None], np.arange(width)[None, :]
    angle = 2.0 * np.pi * (j * m % width) / width
    scale = 1.0 / math.sqrt(width)
    tables = split_const(np.cos(angle) * scale) + split_const(np.sin(angle) * scale)
    per_slot = width // LANES
    whole = lambda shape: pl.BlockSpec(shape, lambda i: (0, 0))
    out = pl.pallas_call(
        fine_kernel,
        grid=(slot_chunks,),
        out_shape=jax.ShapeDtypeStruct((2, slot_chunks * slots * per_slot, LANES), jnp.float32),
        in_specs=[
            pl.BlockSpec((sources, 1, 2, rows, slots), lambda i: (0, i, 0, 0, 0)),
            whole(fine_taps.shape),
        ]
        + [whole((length, width))] * 4,
        out_specs=pl.BlockSpec((2, slots * per_slot, LANES), lambda i: (0, i, 0)),
        name="fine",
    )(arrived, fine_taps, *tables)
    return out.reshape(2, 1, slot_chunks * slots, 1, width)


def fine_general(series, fine_taps):
    slots, total_len = series.shape[1:]
    tap_count, width = fine_taps.shape
    frames = -(-total_len // width)
    blocks = jnp.pad(series, ((0, 0), (0, 0), (0, frames * width - total_len)))
    blocks = blocks.reshape(2, slots, frames, width)
    filtered = fine_taps[0] * blocks
    for k in range(1, min(tap_count, frames)):
        term = fine_taps[k] * blocks[:, :, k:]
        filtered = filtered + jnp.pad(term, ((0, 0), (0, 0), (0, k), (0, 0)))
    j, m = np.arange(width)[:, None], np.arange(width)[None, :]
    angle = 2.0 * np.pi * (j * m % width) / width
    scale = 1.0 / math.sqrt(width)
    cos = jnp.asarray((np.cos(angle) * scale).astype(np.float32))
    sin = jnp.asarray((np.sin(angle) * scale).astype(np.float32))
    product = partial(jnp.einsum, "snfj,jm->snfm", precision=lax.Precision.HIGHEST)
    with_cos, with_sin = product(filtered, cos), product(filtered, sin)
    return jnp.stack([with_cos[0] + with_sin[1], with_cos[1] - with_sin[0]])[:, None]


def body(signal, coarse_taps, fine_taps, channel_order):
    signal = signal[:, 0]
    slab_len, width = signal.shape[1:]
    tap_count = coarse_taps.shape[0]
    chunks = width // LANES
    owners = lax.axis_size(GROUP)
    own_count = width // owners
    place = channel_order.reshape(chunks, LANES)
    lead = -(-(tap_count - 1) // ROWS) * ROWS
    total_len = owners * slab_len
    if own_count % LANES == 0 and total_len <= fine_taps.shape[1] and slab_len % ROWS == 0 and lead <= slab_len:
        arrived = coarse_exchange(signal, coarse_taps, place)
        return fine_local(arrived.reshape(-1, *arrived.shape[2:]), fine_taps)
    next_rows = shifted(signal[:, :lead], GROUP, -1)
    ordered = coarse_local(signal, next_rows, coarse_taps, place)
    blocks = ordered.transpose(0, 3, 1, 2).reshape(owners, own_count, 2, slab_len)
    arrived = lax.all_to_all(blocks, GROUP, split_axis=0, concat_axis=0, tiled=True)
    series = arrived.transpose(2, 1, 0, 3).reshape(2, own_count, total_len)
    return fine_general(series, fine_taps)


def solution(mesh):
    in_specs = (P(None, "pol", ("beam", "tm", "sect"), None), P(), P(), P())
    out_specs = P(None, "pol", ("beam", "tm", "sect"), None, None)
    return jax.shard_map(body, mesh=mesh, in_specs=in_specs, out_specs=out_specs, check_vma=False)
```

```python
from functools import partial
import math

import jax
import jax.numpy as jnp
import numpy as np
from jax import lax
from jax.experimental import pallas as pl
from jax.experimental.pallas import tpu as pltpu
from jax.sharding import PartitionSpec as P

LANES = 128
ROWS = 8
GROUP = ("tm", "sect")
PHASES = 2


def shifted(value, axis, steps):
    count = lax.axis_size(axis)
    initial, last = (max(0, -steps), min(count, count - steps))
    return lax.ppermute(value, axis, [(source, source + steps) for source in range(initial, last)])


def split_const(table):
    high = np.asarray(table, np.float32).astype(jnp.bfloat16)
    low = (np.asarray(table, np.float64) - high.astype(np.float64)).astype(jnp.bfloat16)
    return high, low


def split(value):
    high = value.astype(jnp.bfloat16)
    low = (value - high.astype(jnp.float32)).astype(jnp.bfloat16)
    return high, low


def dot3(high, low, table_high, table_low):
    product = partial(jnp.dot, preferred_element_type=jnp.float32)
    return product(high, table_high) + (product(low, table_high) + product(high, table_low))


def butterflies(points):
    count = len(points)
    if count == 1:
        return points
    even, odd = butterflies(points[0::2]), butterflies(points[1::2])
    first, second = [], []
    for k in range(count // 2):
        angle = -2.0 * math.pi * k / count
        cos, sin = math.cos(angle), math.sin(angle)
        (er, ei), (xr, xi) = even[k], odd[k]
        if k == 0:
            tr, ti = xr, xi
        elif 4 * k == count:
            tr, ti = xi, -xr
        else:
            tr, ti = xr * cos - xi * sin, xr * sin + xi * cos
        first.append((er + tr, ei + ti))
        second.append((er - tr, ei - ti))
    return first + second


def coarse_tables(width):
    chunks = width // LANES
    k, b = np.arange(chunks)[:, None], np.arange(LANES)[None, :]
    angle = 2.0 * np.pi * (k * b % width) / width
    twist = np.stack([np.cos(angle), -np.sin(angle)]).astype(np.float32)
    b, m = np.arange(LANES)[:, None], np.arange(LANES)[None, :]
    angle = 2.0 * np.pi * (b * m % LANES) / LANES
    cos, sin = np.cos(angle), np.sin(angle)
    matrix = np.block([[cos, -sin], [sin, cos]]) / math.sqrt(width)
    high, low = split_const(matrix)
    return twist, high, low


def fill(ext, source, first_row):
    chunks = ext.shape[1]
    rows = source.shape[1]
    for q in range(chunks):
        for c in range(2):
            ext[c, q, first_row : first_row + rows, :] = source[c, :, q * LANES : (q + 1) * LANES]


def spectra_rows(ext, taps_ref, twist_ref, high_ref, low_ref, filt, lhs, spec, start, rows):
    chunks = ext.shape[1]
    tap_count = taps_ref.shape[0]
    groups = rows // ROWS

    @pl.loop(0, chunks)
    def _(q):
        lanes = pl.ds(pl.multiple_of(q * LANES, LANES), LANES)
        sums = [[None] * groups for _ in range(2)]
        for k in range(tap_count):
            tap = jnp.broadcast_to(taps_ref[k : k + 1, lanes], (ROWS, LANES))
            for c in range(2):
                for g in range(groups):
                    term = tap * ext[c, q, start + g * ROWS + k : start + (g + 1) * ROWS + k, :]
                    sums[c][g] = term if k == 0 else sums[c][g] + term
        for c in range(2):
            for g in range(groups):
                filt[c, q, start + g * ROWS : start + (g + 1) * ROWS, :] = sums[c][g]

    @pl.loop(0, groups)
    def _(g):
        at = pl.ds(pl.multiple_of(start + g * ROWS, ROWS), ROWS)
        points = [(filt[0, q, at, :], filt[1, q, at, :]) for q in range(chunks)]
        for k, (re, im) in enumerate(butterflies(points)):
            wr, wi = twist_ref[0, k : k + 1, :], twist_ref[1, k : k + 1, :]
            lhs[k, at, 0:LANES] = re * wr - im * wi
            lhs[k, at, LANES : 2 * LANES] = re * wi + im * wr

    @pl.loop(0, chunks // 8)
    def _(j):
        part = pl.ds(j * 8, 8)
        value = lhs[part, start : start + rows, :].reshape(8 * rows, 2 * LANES)
        high, low = split(value)
        result = dot3(high, low, high_ref[...], low_ref[...])
        spec[part, start : start + rows, :] = result.reshape(8, rows, 2 * LANES)


def gathered(spec, place_ref, p, start, rows):
    chunks = spec.shape[0]
    channel = jnp.broadcast_to(place_ref[pl.ds(p, 1), :], (ROWS, LANES))
    lane = lax.div(channel, chunks)
    chunk = channel - lane * chunks
    keys = [(c, g) for c in range(2) for g in range(rows // ROWS)]
    sums = {}
    for q in range(chunks):
        mask = chunk == q
        for c, g in keys:
            source = spec[q, start + g * ROWS : start + (g + 1) * ROWS, c * LANES : (c + 1) * LANES]
            moved = jnp.take_along_axis(source, lane, axis=1, mode="promise_in_bounds")
            sums[c, g] = moved if q == 0 else jnp.where(mask, moved, sums[c, g])
    return sums


def coarse_kernel(signal_ref, next_ref, taps_ref, place_ref, twist_ref, high_ref, low_ref, out_ref, ext, filt, lhs, spec):
    rows = signal_ref.shape[1]
    fill(ext, signal_ref, 0)
    fill(ext, next_ref, rows)
    spectra_rows(ext, taps_ref, twist_ref, high_ref, low_ref, filt, lhs, spec, 0, rows)
    chunks = spec.shape[0]

    @pl.loop(0, chunks)
    def _(p):
        sums = gathered(spec, place_ref, p, 0, rows)
        for (c, g), value in sums.items():
            out_ref[p, c, g * ROWS : (g + 1) * ROWS, :] = value


def coarse_local(signal, next_rows, taps, place):
    _, rows, width = signal.shape
    chunks = width // LANES
    twist, high, low = coarse_tables(width)
    lead = next_rows.shape[1]
    return pl.pallas_call(
        coarse_kernel,
        out_shape=jax.ShapeDtypeStruct((chunks, 2, rows, LANES), jnp.float32),
        in_specs=[pl.BlockSpec(memory_space=pltpu.VMEM)] * 7,
        out_specs=pl.BlockSpec(memory_space=pltpu.VMEM),
        scratch_shapes=[
            pltpu.VMEM((2, chunks, rows + lead, LANES), jnp.float32),
            pltpu.VMEM((2, chunks, rows, LANES), jnp.float32),
            pltpu.VMEM((chunks, rows, 2 * LANES), jnp.float32),
            pltpu.VMEM((chunks, rows, 2 * LANES), jnp.float32),
        ],
        name="coarse",
    )(signal, next_rows, taps, place, twist, high, low)


def exchange_kernel(
    signal_ref, taps_ref, place_ref, twist_ref, high_ref, low_ref, out_ref,
    halo, ext, filt, lhs, spec, stage, halo_send, halo_recv, send_sem, recv_sem, own_sem,
):
    tms, sects = lax.axis_size("tm"), lax.axis_size("sect")
    owners = tms * sects
    tm, sect = lax.axis_index("tm"), lax.axis_index("sect")
    me = tm * sects + sect
    chunks = spec.shape[0]
    slot_chunks = chunks // owners
    slab_len = signal_ref.shape[1]
    rows = slab_len // PHASES
    lead = halo.shape[1]

    def device(index):
        return {"tm": lax.div(index, sects), "sect": lax.rem(index, sects)}

    barrier = pltpu.get_barrier_semaphore()
    for offset in range(1, owners):
        peer = lax.rem(me + offset, owners)
        pl.semaphore_signal(barrier, inc=1, device_id=device(peer), device_id_type=pl.DeviceIdType.MESH)
    pl.semaphore_wait(barrier, owners - 1)

    halo_copy = pltpu.make_async_remote_copy(
        src_ref=signal_ref.at[:, 0:lead, :],
        dst_ref=halo,
        send_sem=halo_send,
        recv_sem=halo_recv,
        device_id=device(lax.rem(me + owners - 1, owners)),
        device_id_type=pl.DeviceIdType.MESH,
    )

    @pl.when(me > 0)
    def _():
        halo_copy.start()

    def block_copy(phase, owner, source):
        return pltpu.make_async_remote_copy(
            src_ref=stage.at[owner, phase],
            dst_ref=out_ref.at[source, phase],
            send_sem=send_sem.at[phase, owner],
            recv_sem=recv_sem.at[phase, source],
            device_id=device(owner),
            device_id_type=pl.DeviceIdType.MESH,
        )

    fill(ext, signal_ref, 0)
    for phase in range(PHASES):
        start = phase * rows
        if phase == PHASES - 1:

            @pl.when(me < owners - 1)
            def _():
                halo_copy.wait_recv()
                fill(ext, halo, slab_len)

            @pl.when(me == owners - 1)
            def _():
                ext[:, :, slab_len:, :] = jnp.zeros((2, chunks, lead, LANES), jnp.float32)

        spectra_rows(ext, taps_ref, twist_ref, high_ref, low_ref, filt, lhs, spec, start, rows)

        @pl.loop(0, owners)
        def _(step):
            turn = lax.div(step, sects)
            half = tms // 2
            turn = jnp.where(turn < tms - half, half + turn, tms - 1 - turn)
            owner = lax.rem(tm + turn, tms) * sects + lax.rem(sect + 1 + step, sects)

            @pl.loop(0, slot_chunks)
            def _(i):
                sums = gathered(spec, place_ref, owner * slot_chunks + i, start, rows)
                for (c, g), value in sums.items():
                    stage[owner, phase, i, c, g * ROWS : (g + 1) * ROWS, :] = value

            @pl.when(owner != me)
            def _():
                block_copy(phase, owner, me).start()

    own_copy = pltpu.make_async_copy(stage.at[me], out_ref.at[me], own_sem)
    own_copy.start()
    own_copy.wait()

    @pl.when(me > 0)
    def _():
        halo_copy.wait_send()

    for phase in range(PHASES):

        @pl.loop(1, owners)
        def _(offset):
            peer = lax.rem(me + offset, owners)
            copy = block_copy(phase, peer, peer)
            copy.wait_send()
            copy.wait_recv()


def coarse_exchange(signal, taps, place):
    _, rows, width = signal.shape
    chunks = width // LANES
    owners = lax.axis_size(GROUP)
    twist, high, low = coarse_tables(width)
    lead = rows // PHASES
    blocks = (owners, PHASES, chunks // owners, 2, lead, LANES)
    return pl.pallas_call(
        exchange_kernel,
        out_shape=jax.ShapeDtypeStruct(blocks, jnp.float32),
        in_specs=[pl.BlockSpec(memory_space=pltpu.VMEM)] * 6,
        out_specs=pl.BlockSpec(memory_space=pl.ANY),
        scratch_shapes=[
            pltpu.VMEM((2, lead, width), jnp.float32),
            pltpu.VMEM((2, chunks, rows + lead, LANES), jnp.float32),
            pltpu.VMEM((2, chunks, rows, LANES), jnp.float32),
            pltpu.VMEM((chunks, rows, 2 * LANES), jnp.float32),
            pltpu.VMEM((chunks, rows, 2 * LANES), jnp.float32),
            pltpu.VMEM(blocks, jnp.float32),
            pltpu.SemaphoreType.DMA,
            pltpu.SemaphoreType.DMA,
            pltpu.SemaphoreType.DMA((PHASES, owners)),
            pltpu.SemaphoreType.DMA((PHASES, owners)),
            pltpu.SemaphoreType.DMA,
        ],
        compiler_params=pltpu.CompilerParams(collective_id=0, has_side_effects=True),
        name="exchange",
    )(signal, taps, place, twist, high, low)


def fine_kernel(arrived_ref, taps_ref, even_high, even_low, odd_high, odd_low, out_ref, series):
    sources, slot_chunks, _, rows, slots = arrived_ref.shape
    length = sources * rows
    half = even_high.shape[1] // 2
    per_slot = 2 * half // LANES
    taps = taps_ref[:, :length].T[:, 0:1]
    for i in range(slot_chunks):
        for c in range(2):
            series[i, c] = arrived_ref[:, i, c].reshape(length, slots) * taps
    sums = []
    for parity, (table_high, table_low) in enumerate(((even_high, even_low), (odd_high, odd_low))):
        at = pl.ds(parity, length // 2, stride=2)
        value = jnp.concatenate(
            [jnp.concatenate([series[i, c, at, :].T for c in range(2)], axis=1) for i in range(slot_chunks)], axis=0
        )
        high, low = split(value)
        product = partial(jnp.dot, preferred_element_type=jnp.float32)
        both = product(jnp.concatenate([high, low], axis=0), table_high[...])
        count = slot_chunks * slots
        sums.append(both[:count] + (both[count:] + product(high, table_low[...])))
    for c in range(2):
        for h in range(half // LANES):
            lanes = slice(c * half + h * LANES, c * half + (h + 1) * LANES)
            even, odd = sums[0][:, lanes], sums[1][:, lanes]
            out_ref[c, pl.ds(h, slot_chunks * slots, stride=per_slot), :] = even + odd
            out_ref[c, pl.ds(h + half // LANES, slot_chunks * slots, stride=per_slot), :] = even - odd


def fine_local(arrived, fine_taps):
    sources, slot_chunks, _, rows, slots = arrived.shape
    length = sources * rows
    width = fine_taps.shape[1]
    tables = []
    for parity in range(2):
        j, m = np.arange(parity, length, 2)[:, None], np.arange(width // 2)[None, :]
        angle = 2.0 * np.pi * (j * m % width) / width
        cos, sin = np.cos(angle), np.sin(angle)
        tables += split_const(np.block([[cos, -sin], [sin, cos]]) / math.sqrt(width))
    per_slot = width // LANES
    step = 2 if slot_chunks % 2 == 0 else 1
    whole = lambda shape: pl.BlockSpec(shape, lambda i: (0, 0))
    out = pl.pallas_call(
        fine_kernel,
        grid=(slot_chunks // step,),
        out_shape=jax.ShapeDtypeStruct((2, slot_chunks * slots * per_slot, LANES), jnp.float32),
        in_specs=[
            pl.BlockSpec((sources, step, 2, rows, slots), lambda i: (0, i, 0, 0, 0)),
            whole(fine_taps.shape),
        ]
        + [whole((length, width))] * 4,
        out_specs=pl.BlockSpec((2, step * slots * per_slot, LANES), lambda i: (0, i, 0)),
        scratch_shapes=[pltpu.VMEM((step, 2, length, slots), jnp.float32)],
        name="fine",
    )(arrived, fine_taps, *tables)
    return out.reshape(2, 1, slot_chunks * slots, 1, width)


def fine_general(series, fine_taps):
    slots, total_len = series.shape[1:]
    tap_count, width = fine_taps.shape
    frames = -(-total_len // width)
    blocks = jnp.pad(series, ((0, 0), (0, 0), (0, frames * width - total_len)))
    blocks = blocks.reshape(2, slots, frames, width)
    filtered = fine_taps[0] * blocks
    for k in range(1, min(tap_count, frames)):
        term = fine_taps[k] * blocks[:, :, k:]
        filtered = filtered + jnp.pad(term, ((0, 0), (0, 0), (0, k), (0, 0)))
    j, m = np.arange(width)[:, None], np.arange(width)[None, :]
    angle = 2.0 * np.pi * (j * m % width) / width
    scale = 1.0 / math.sqrt(width)
    cos = jnp.asarray((np.cos(angle) * scale).astype(np.float32))
    sin = jnp.asarray((np.sin(angle) * scale).astype(np.float32))
    product = partial(jnp.einsum, "snfj,jm->snfm", precision=lax.Precision.HIGHEST)
    with_cos, with_sin = product(filtered, cos), product(filtered, sin)
    return jnp.stack([with_cos[0] + with_sin[1], with_cos[1] - with_sin[0]])[:, None]


def body(signal, coarse_taps, fine_taps, channel_order):
    signal = signal[:, 0]
    slab_len, width = signal.shape[1:]
    tap_count = coarse_taps.shape[0]
    chunks = width // LANES
    owners = lax.axis_size(GROUP)
    own_count = width // owners
    place = channel_order.reshape(chunks, LANES)
    lead = -(-(tap_count - 1) // ROWS) * ROWS
    total_len = owners * slab_len
    if own_count % LANES == 0 and total_len <= fine_taps.shape[1] and slab_len == PHASES * lead:
        arrived = coarse_exchange(signal, coarse_taps, place)
        return fine_local(arrived.reshape(-1, *arrived.shape[2:]), fine_taps)
    next_rows = shifted(signal[:, :lead], GROUP, -1)
    ordered = coarse_local(signal, next_rows, coarse_taps, place)
    blocks = ordered.transpose(0, 3, 1, 2).reshape(owners, own_count, 2, slab_len)
    arrived = lax.all_to_all(blocks, GROUP, split_axis=0, concat_axis=0, tiled=True)
    series = arrived.transpose(2, 1, 0, 3).reshape(2, own_count, total_len)
    return fine_general(series, fine_taps)


def solution(mesh):
    in_specs = (P(None, "pol", ("beam", "tm", "sect"), None), P(), P(), P())
    out_specs = P(None, "pol", ("beam", "tm", "sect"), None, None)
    return jax.shard_map(body, mesh=mesh, in_specs=in_specs, out_specs=out_specs, check_vma=False)
```
